256 devices in a mesh: dp: 8 (over z_lo, core), vocab: 32 (over z_hi, x, y).
Axes of the slice: x: 4, y: 4, z: 8 (z_hi: 2, z_lo: 4; z = z_hi * 4 + z_lo), core: 2. Of those that a mesh axis runs over, the one named last changes fastest.
Arguments:
- policy_hidden: bfloat16 [1024, 4096], P('dp'), may hold values from -84 to 84
- policy_weight: bfloat16 [4096, 65536], P('dp', 'vocab'), may hold values from -0.09375 to 0.09375
- reference_hidden: bfloat16 [1024, 4096], P(('dp', 'vocab')), may hold values from -84 to 84
- reference_weight: bfloat16 [4096, 65536], P(None, ('dp', 'vocab')), may hold values from -0.09375 to 0.09375
- targets: int32 [1024], replicated, may hold values from 0 to 65535
- response_mask: int32 [1024], replicated, may hold values 0 or 1
- pair_index: int32 [32], replicated, may hold values from 0 to 31, each once
Outputs:
- hidden_grad: bfloat16 [1024, 4096], P('vocab', 'dp')
- weight_grad: bfloat16 [4096, 65536], P('dp', 'vocab')
- total_loss: float32 [], replicated
The draws below stay inside these ranges and needn't reach their ends.
Inputs may be any that keep to these rules, and one draw needn't show every extreme that they name: `pair_index`: each number of 0 to 31 once; entries 2p and 2p + 1 are the chosen and the rejected sequence of pair p.
All inputs are finite; a program needn't handle non-finite values.
Results may differ from the reference program's by a relative error of at most 0.005.
The reference program's roundings to bfloat16 on the way (of `logit_grad`) count: a program that leaves them out, or rounds other values in their place, can miss the bound.
Values may be sent and summed in bfloat16 or wider, within the bound.
No kernel may reach another device: no remote copies, remote signals or barrier semaphores. Data moves between devices by JAX's collectives and lax.ppermute only.
A program may use at most 128 MiB of HBM per device.

```python
import math
import jax
import jax.numpy as jnp
import numpy as np
from jax import lax

D = 4096
VOCAB = 65536
SEQ_LEN = 32
SEQS = 32
TOKENS = 1024


def scaled_rows(key, salt):
    folded = jax.random.fold_in(key, salt)
    key_value = jax.random.fold_in(folded, 1)
    return 3.0 * jnp.clip(jax.random.normal(key_value, (TOKENS, D), jnp.float32), -6.0, 6.0)


def draw_policy_hidden(key, part):
    return scaled_rows(key, 11).astype(jnp.bfloat16)


def draw_reference_hidden(key, part):
    return scaled_rows(key, 23).astype(jnp.bfloat16)


def touch_ends(array, stream_key, smallest, top_value):
    longest = array.shape.index(max(array.shape))
    spots = []
    for shift in (0, 1):
        where = [jax.random.randint(jax.random.fold_in(stream_key, axis), (), 0, length) for axis, length in enumerate(array.shape)]
        where[longest] = (where[longest] + shift) % array.shape[longest]
        spots.append(tuple(where))
    return array.at[spots[0]].set(smallest).at[spots[1]].set(top_value)


def levels(stream_key, shape, cuts, least, high):
    def one(axis_at, parts):
        steps = jax.random.uniform(jax.random.fold_in(jax.random.fold_in(stream_key, 6), axis_at), (parts,), jnp.float32, least / len(cuts), high / len(cuts))
        return jnp.repeat(jnp.exp(steps), shape[axis_at] // parts).reshape((-1,) + (1,) * (len(shape) - axis_at - 1))

    level = one(*cuts[0])
    for cut in cuts[1:]:
        level = level * one(*cut)
    return level


def rank_bounds(amount, skew):
    weights = [(1 << 20) // math.isqrt(standing ** skew) + 1 for standing in range(1, amount + 1)]
    scale = 1 + sum(weights) // (1 << 30)
    return np.cumsum(np.array([max(1, weight // scale) for weight in weights]))


def skewed_ids(stream_key, dims, amount, slope):
    listing = rank_bounds(amount, slope)
    lot = jax.random.randint(jax.random.fold_in(stream_key, 1), dims, 0, int(listing[amount - 1]))
    standing = jnp.searchsorted(jnp.asarray(listing, jnp.int32), lot, side="right")
    return jax.random.permutation(jax.random.fold_in(stream_key, 2), amount)[standing].astype(jnp.int32)


def scatter_about(key, dims, scale, reach, shards=(), kind=jnp.bfloat16):
    array = jax.random.normal(key, dims, jnp.float32) * scale
    if len(shards) > 0:
        array = levels(key, dims, shards, -0.22, 0.18) * array
    return jnp.clip(array, min=-reach, max=reach).astype(kind)


def setup_inputs(seed: int = 0) -> dict:
    key_of = jax.random.split(jax.random.key(seed), 8)
    policy_hidden = draw_policy_hidden(jax.random.fold_in(key_of[7], 71), 0)
    policy_weight = scatter_about(key_of[1], (D, VOCAB), D ** -0.5, 0.09375, ((0, 8), (1, 32)))
    reference_hidden = draw_reference_hidden(jax.random.fold_in(key_of[7], 71), 0)
    reference_weight = scatter_about(key_of[3], (D, VOCAB), D ** -0.5, 0.09375, ((1, 256),))
    targets = touch_ends(skewed_ids(key_of[4], (TOKENS,), VOCAB, 2), jax.random.fold_in(key_of[4], 3), 0, VOCAB - 1).astype(jnp.int32)
    response_mask = touch_ends((jax.random.randint(key_of[5], (TOKENS,), 0, 4) < 3).astype(jnp.int32), jax.random.fold_in(key_of[5], 1), 0, 1)
    pair_index = jax.random.permutation(key_of[6], SEQS).astype(jnp.int32)
    return {"policy_hidden": policy_hidden, "policy_weight": policy_weight, "reference_hidden": reference_hidden, "reference_weight": reference_weight, "targets": targets, "response_mask": response_mask, "pair_index": pair_index}


beta = 0.1
loss_scale = 4096.0
block_size = 64


def pair_terms(log_ratio, pair_index):
    chosen = pair_index[0::2]
    rejected = pair_index[1::2]
    margin = beta * (log_ratio[chosen] - log_ratio[rejected])
    pair_count = chosen.shape[0]
    total_loss = jnp.sum(jax.nn.softplus(-margin)) / pair_count
    weight = -beta * loss_scale * jax.nn.sigmoid(-margin) / pair_count
    numbers = jnp.arange(log_ratio.shape[0], dtype=jnp.int32)[:, None]
    factor = jnp.sum(jnp.where(numbers == chosen[None, :], weight[None, :], 0.0) - jnp.where(numbers == rejected[None, :], weight[None, :], 0.0), axis=1)
    return total_loss, factor


def token_logp(hidden, weight, targets):
    blocks = hidden.shape[0] // block_size

    def block_logp(inputs):
        row_block, target_block = inputs
        logits = jnp.dot(row_block, weight, preferred_element_type=jnp.float32)
        largest = jnp.max(logits, axis=1)
        exp_total = jnp.sum(jnp.exp(logits - largest[:, None]), axis=1)
        picked = jnp.take_along_axis(logits, target_block[:, None], axis=1)[:, 0]
        return picked - largest - jnp.log(exp_total)

    return lax.map(block_logp, (hidden.reshape(blocks, block_size, hidden.shape[1]), targets.reshape(blocks, block_size))).reshape(-1)


def reference(policy_hidden, policy_weight, reference_hidden, reference_weight, targets, response_mask, pair_index):
    policy_logp = token_logp(policy_hidden, policy_weight, targets)
    reference_logp = token_logp(reference_hidden, reference_weight, targets)
    active = response_mask.astype(jnp.float32)
    log_ratio = jnp.sum((active * (policy_logp - reference_logp)).reshape(-1, SEQ_LEN), axis=1)
    total_loss, factor = pair_terms(log_ratio, pair_index)
    token_scale = active * jnp.repeat(factor, SEQ_LEN)
    blocks = policy_hidden.shape[0] // block_size
    vocab_ids = lax.broadcasted_iota(jnp.int32, (block_size, policy_weight.shape[1]), 1)

    def backward(weight_grad, inputs):
        row_block, target_block, scale_block = inputs
        logits = jnp.dot(row_block, policy_weight, preferred_element_type=jnp.float32)
        largest = jnp.max(logits, axis=1, keepdims=True)
        log_total = largest + jnp.log(jnp.sum(jnp.exp(logits - largest), axis=1, keepdims=True))
        onehot = (vocab_ids == target_block[:, None]).astype(jnp.float32)
        logit_grad = (scale_block[:, None] * (onehot - jnp.exp(logits - log_total))).astype(jnp.bfloat16)
        weight_grad = weight_grad + jnp.dot(row_block.T, logit_grad, preferred_element_type=jnp.float32)
        row_grad = jnp.dot(logit_grad, policy_weight.T, preferred_element_type=jnp.float32).astype(jnp.bfloat16)
        return weight_grad, row_grad

    weight_grad, hidden_grad = lax.scan(backward, jnp.zeros(policy_weight.shape, jnp.float32), (policy_hidden.reshape(blocks, block_size, policy_hidden.shape[1]), targets.reshape(blocks, block_size), token_scale.reshape(blocks, block_size)))
    return hidden_grad.reshape(policy_hidden.shape), weight_grad.astype(jnp.bfloat16), total_loss
```

```python
import jax
import jax.numpy as jnp
from jax import lax
from jax.sharding import Mesh
from jax.sharding import PartitionSpec as P

AXES = ("zl", "c", "zh", "x", "y")
DP = ("zl", "c")
VOCAB = ("zh", "x", "y")
DP_VOCAB = ("zl", "c", "zh", "x", "y")
RING = ("zl", "zh")

beta = 0.1
loss_scale = 4096.0


def swap(value, axis, k):
    n = lax.axis_size(axis)
    return lax.ppermute(value, axis, [(i, i ^ k) for i in range(n)])


def from_ahead(value, axis, k):
    n = lax.axis_size(axis)
    return lax.ppermute(value, axis, [(i, (i - k) % n) for i in range(n)])


def from_z_ahead(value, k):
    at = lambda z: (z % 4) * 2 + z // 4
    return lax.ppermute(value, RING, [(at(z), at((z - k) % 8)) for z in range(8)])


def placed(pieces, first):
    out = jnp.zeros((4, *pieces[0].shape), pieces[0].dtype)
    for k, piece in enumerate(pieces):
        out = lax.dynamic_update_slice_in_dim(out, piece[None], (first + k) % 4, 0)
    return out


def gathered(value, axis):
    pieces = [value] + [from_ahead(value, axis, k) for k in (1, 2, 3)]
    return placed(pieces, lax.axis_index(axis))


def gathered_z(value):
    pieces = [value] + [from_z_ahead(value, k) for k in (1, 2, -1)]
    return placed(pieces, lax.axis_index("zl"))


def plane(value):
    upper = gathered(gathered(value[:2], "x"), "y")
    lower = gathered(gathered(value[2:], "y"), "x")
    return upper, lower


def pair_terms(log_ratio, pair_index):
    chosen = pair_index[0::2]
    rejected = pair_index[1::2]
    margin = beta * (log_ratio[chosen] - log_ratio[rejected])
    pair_count = chosen.shape[0]
    total_loss = jnp.sum(jax.nn.softplus(-margin)) / pair_count
    weight = -beta * loss_scale * jax.nn.sigmoid(-margin) / pair_count
    numbers = jnp.arange(log_ratio.shape[0], dtype=jnp.int32)[:, None]
    factor = jnp.sum(
        jnp.where(numbers == chosen[None, :], weight[None, :], 0.0)
        - jnp.where(numbers == rejected[None, :], weight[None, :], 0.0),
        axis=1,
    )
    return (total_loss, factor)


def head_stats(logits, targets, offset):
    top = jnp.max(logits, axis=1)
    exp_total = jnp.sum(jnp.exp(logits - top[:, None]), axis=1)
    ids = lax.broadcasted_iota(jnp.int32, logits.shape, 1)
    pick = jnp.sum(jnp.where(ids == (targets - offset)[:, None], logits, 0.0), axis=1)
    return (top, exp_total, pick)


def merge(a, b):
    top = jnp.maximum(a[0], b[0])
    return (top, a[1] * jnp.exp(a[0] - top) + b[1] * jnp.exp(b[0] - top), a[2] + b[2])


def merge_heads(a, b):
    p = merge(a[0:3], b[0:3])
    r = merge(a[3:6], b[3:6])
    return jnp.stack(p + r)


def merged_over(stats, axis):
    if lax.axis_size(axis) == 2:
        return merge_heads(stats, swap(stats, axis, 1))
    others = [swap(stats, axis, k) for k in (1, 2, 3)]
    return merge_heads(merge_heads(stats, others[0]), merge_heads(others[1], others[2]))


def local(
    policy_hidden,
    policy_weight,
    reference_hidden,
    reference_weight,
    targets,
    response_mask,
    pair_index,
):
    zl, c, zh, x, y = (lax.axis_index(a) for a in AXES)
    width = policy_weight.shape[1] // 4
    rows = policy_weight.shape[0]

    def mine(values):
        return lax.dynamic_index_in_dim(values.reshape(4, 2, 128), c, 1, keepdims=False).reshape(-1)

    my_targets = mine(targets)
    active = mine(response_mask).astype(jnp.float32)

    own = lax.dynamic_slice_in_dim(policy_hidden, (x * 4 + y) * 8, 8, 0)
    own = own.reshape(8, 4, 2, 512)
    first = jnp.where(c == 0, own[:, :, 0], own[:, :, 1]).reshape(8, 2048)
    second = jnp.where(c == 0, own[:, :, 1], own[:, :, 0]).reshape(8, 2048)
    own = jnp.concatenate([first, second], axis=1)
    far = swap(reference_hidden, "zh", 1)
    low = jnp.where(zh == 0, reference_hidden, far)
    high = jnp.where(zh == 0, far, reference_hidden)
    both = gathered_z(jnp.concatenate([own, low, high], axis=0))

    near_weight = lax.all_to_all(policy_weight, "zl", split_axis=1, concat_axis=0, tiled=True)
    far_weight = swap(near_weight, "c", 1)
    other_reference = swap(reference_weight, "c", 1)

    upper, lower = plane(both[:, :8])
    hidden = jnp.concatenate(
        [upper.transpose(2, 1, 0, 3, 4), lower.transpose(2, 0, 1, 3, 4)], axis=0
    ).reshape(512, -1)
    r_upper, r_lower = plane(both[:, 8:])
    r_hidden = jnp.concatenate([r_upper.reshape(256, -1), r_lower.reshape(256, -1)], axis=0)

    def natural(stat):
        a = stat[:256].reshape(4, 4, 2, 2, 4).transpose(2, 3, 1, 0, 4)
        b = stat[256:].reshape(4, 4, 2, 2, 4).transpose(2, 3, 0, 1, 4)
        return jnp.concatenate([a, b], axis=0).reshape(-1)

    t = my_targets.reshape(4, 2, 4, 4, 4)
    r_targets = jnp.concatenate(
        [t[:2].transpose(3, 2, 0, 1, 4).reshape(-1), t[2:].transpose(2, 3, 0, 1, 4).reshape(-1)]
    )

    logits = jnp.dot(
        hidden[:, :2048], near_weight, preferred_element_type=jnp.float32
    ) + jnp.dot(hidden[:, 2048:], far_weight, preferred_element_type=jnp.float32)
    vocab_index = zh * 16 + x * 4 + y
    offset = vocab_index * (4 * width) + zl * width
    policy_stats = head_stats(logits, my_targets, offset)

    reference_width = reference_weight.shape[1]
    near_logits = jnp.dot(r_hidden, reference_weight, preferred_element_type=jnp.float32)
    far_logits = jnp.dot(r_hidden, other_reference, preferred_element_type=jnp.float32)
    near_offset = ((zl * 2 + c) * 32 + vocab_index) * reference_width
    far_offset = ((zl * 2 + 1 - c) * 32 + vocab_index) * reference_width
    reference_stats = merge(
        head_stats(near_logits, r_targets, near_offset),
        head_stats(far_logits, r_targets, far_offset),
    )
    stats = jnp.stack(policy_stats + tuple(natural(s) for s in reference_stats))
    for axis in ("zl", "x", "y", "zh"):
        stats = merged_over(stats, axis)

    policy_total = stats[0] + jnp.log(stats[1])
    reference_logp = stats[5] - stats[3] - jnp.log(stats[4])
    ratio = jnp.sum(
        (active * (stats[2] - policy_total - reference_logp)).reshape(16, 32), axis=1
    )
    far_ratio = swap(ratio, "c", 1)
    ratios = jnp.stack(
        [jnp.where(c == 0, ratio, far_ratio).reshape(4, 4), jnp.where(c == 0, far_ratio, ratio).reshape(4, 4)],
        axis=1,
    ).reshape(32)
    total_loss, factor = pair_terms(ratios, pair_index)
    my_factor = lax.dynamic_index_in_dim(factor.reshape(4, 2, 4), c, 1, keepdims=False).reshape(16)
    token_scale = active * jnp.repeat(my_factor, 32)

    ids = lax.broadcasted_iota(jnp.int32, logits.shape, 1)
    onehot = (ids == (my_targets - offset)[:, None]).astype(jnp.float32)
    logit_grad = (
        token_scale[:, None] * (onehot - jnp.exp(logits - policy_total[:, None]))
    ).astype(jnp.bfloat16)

    beside = swap(logit_grad, "zl", 1)
    across = swap(logit_grad, "zl", 2)
    both_away = swap(across, "zl", 1)
    whole = jnp.zeros((512, 4 * width), jnp.bfloat16)
    for k, piece in enumerate((logit_grad, beside, across, both_away)):
        whole = lax.dynamic_update_slice_in_dim(whole, piece, (zl ^ k) * width, 1)
    other = swap(whole, "c", 1)

    columns = lax.dynamic_slice_in_dim(hidden, zl * rows, rows, 1)
    far_columns = swap(lax.dynamic_slice_in_dim(hidden, 2048 + zl * rows, rows, 1), "c", 1)

    def hidden_of(grad):
        return lax.dot_general(
            grad, policy_weight, (((1,), (1,)), ((), ())), preferred_element_type=jnp.float32
        )

    def weight_of(cols, grad):
        return lax.dot_general(
            cols, grad, (((0,), (0,)), ((), ())), preferred_element_type=jnp.float32
        )

    near_part = hidden_of(whole)
    far_part = hidden_of(other)
    part = jnp.stack(
        [
            jnp.where(c == 0, near_part, far_part).reshape(4, 128, rows),
            jnp.where(c == 0, far_part, near_part).reshape(4, 128, rows),
        ],
        axis=1,
    )
    part = part.reshape(2, 4, 4, 32, rows)
    blocks = part.transpose(1, 2, 0, 3, 4).reshape(16, 2, 32, rows)
    blocks = lax.all_to_all(blocks, ("x", "y"), 0, 0, tiled=True)
    summed = jnp.sum(blocks, axis=0)
    kept = lax.dynamic_index_in_dim(summed, zh, 0, keepdims=False)
    sent = lax.dynamic_index_in_dim(summed, 1 - zh, 0, keepdims=False)
    hidden_grad = (kept + swap(sent, "zh", 1)).astype(jnp.bfloat16)
    weight_grad = (weight_of(columns, whole) + weight_of(far_columns, other)).astype(jnp.bfloat16)
    return (hidden_grad, weight_grad, total_loss)


def solution(mesh):
    torus = Mesh(mesh.devices.reshape(4, 2, 2, 4, 4), AXES)
    in_specs = (P(DP, None), P(DP, VOCAB), P(DP_VOCAB, None), P(None, DP_VOCAB), P(), P(), P())
    out_specs = (P(VOCAB, DP), P(DP, VOCAB), P())
    return jax.shard_map(local, mesh=torus, in_specs=in_specs, out_specs=out_specs, check_vma=False)
```

```python
import jax
import jax.numpy as jnp
from jax import lax
from jax.sharding import Mesh
from jax.sharding import PartitionSpec as P

AXES = ("zl", "c", "zh", "x", "y")
DP = ("zl", "c")
VOCAB = ("zh", "x", "y")
DP_VOCAB = ("zl", "c", "zh", "x", "y")
RING = ("zl", "zh")

beta = 0.1
loss_scale = 4096.0


def swap(value, axis, k):
    n = lax.axis_size(axis)
    return lax.ppermute(value, axis, [(i, i ^ k) for i in range(n)])


def from_ahead(value, axis, k):
    n = lax.axis_size(axis)
    return lax.ppermute(value, axis, [(i, (i - k) % n) for i in range(n)])


def from_z_ahead(value, k):
    at = lambda z: (z % 4) * 2 + z // 4
    return lax.ppermute(value, RING, [(at(z), at((z - k) % 8)) for z in range(8)])


def placed(pieces, first):
    out = jnp.zeros((4, *pieces[0].shape), pieces[0].dtype)
    for k, piece in enumerate(pieces):
        out = lax.dynamic_update_slice_in_dim(out, piece[None], (first + k) % 4, 0)
    return out


def gathered(value, axis):
    pieces = [value] + [from_ahead(value, axis, k) for k in (1, 2, 3)]
    return placed(pieces, lax.axis_index(axis))


def gathered_z(value):
    pieces = [value] + [from_z_ahead(value, k) for k in (1, 2, -1)]
    return placed(pieces, lax.axis_index("zl"))


def put(heads, colour, place, start, piece):
    return tuple(
        lax.dynamic_update_slice(
            head, piece[None, None, :, :, 8 * h : 8 * h + 8], (colour, place, start, 0, 0, 0)
        )
        for h, head in enumerate(heads)
    )


def plane(value):
    heads = tuple(jnp.zeros((2, 4, 4, 2, 8, value.shape[2]), value.dtype) for _ in range(2))
    rows = {0: gathered(value[:2], "x"), 1: gathered(value[2:], "y")}
    for colour, axis in ((0, "y"), (1, "x")):
        i = lax.axis_index(axis)
        row = rows[colour]
        ahead = from_ahead(row, axis, 1)
        behind = from_ahead(row, axis, 3)
        low, high = ahead[:2], behind[2:]
        far_low = from_ahead(low, axis, 1)
        far_high = from_ahead(high, axis, 3)
        heads = put(heads, colour, i, 0, row)
        heads = put(heads, colour, (i + 1) % 4, 0, ahead)
        heads = put(heads, colour, (i + 3) % 4, 0, behind)
        heads = put(heads, colour, (i + 2) % 4, 0, far_low)
        heads = put(heads, colour, (i + 2) % 4, 2, far_high)
    return tuple(head.reshape(512, -1) for head in heads)


def pair_terms(log_ratio, pair_index):
    chosen = pair_index[0::2]
    rejected = pair_index[1::2]
    margin = beta * (log_ratio[chosen] - log_ratio[rejected])
    pair_count = chosen.shape[0]
    total_loss = jnp.sum(jax.nn.softplus(-margin)) / pair_count
    weight = -beta * loss_scale * jax.nn.sigmoid(-margin) / pair_count
    numbers = jnp.arange(log_ratio.shape[0], dtype=jnp.int32)[:, None]
    factor = jnp.sum(
        jnp.where(numbers == chosen[None, :], weight[None, :], 0.0)
        - jnp.where(numbers == rejected[None, :], weight[None, :], 0.0),
        axis=1,
    )
    return (total_loss, factor)


def head_stats(logits, targets, offset):
    top = jnp.max(logits, axis=1)
    exp_total = jnp.sum(jnp.exp(logits - top[:, None]), axis=1)
    ids = lax.broadcasted_iota(jnp.int32, logits.shape, 1)
    pick = jnp.sum(jnp.where(ids == (targets - offset)[:, None], logits, 0.0), axis=1)
    return (top, exp_total, pick)


def merge(a, b):
    top = jnp.maximum(a[0], b[0])
    return (top, a[1] * jnp.exp(a[0] - top) + b[1] * jnp.exp(b[0] - top), a[2] + b[2])


def merge_heads(a, b):
    return merge(a[0:3], b[0:3]) + merge(a[3:6], b[3:6])


def exchanged(stats, axis, k, extra=()):
    both = swap(jnp.stack(stats + extra), axis, k)
    rows = tuple(both[n] for n in range(both.shape[0]))
    return merge_heads(stats, rows[:6]), rows[6:]


def local(
    policy_hidden,
    policy_weight,
    reference_hidden,
    reference_weight,
    targets,
    response_mask,
    pair_index,
):
    zl, c, zh, x, y = (lax.axis_index(a) for a in AXES)
    width = policy_weight.shape[1] // 4
    rows = policy_weight.shape[0]

    def mine(values):
        return lax.dynamic_index_in_dim(values.reshape(4, 2, 128), c, 1, keepdims=False)

    def policy_order(v):
        v = v.reshape(4, 4, 4, 8)
        return jnp.concatenate([v[:2].transpose(2, 1, 0, 3), v[2:].transpose(1, 2, 0, 3)]).reshape(-1)

    def from_policy_order(v):
        v = v.reshape(2, 4, 4, 2, 8)
        return jnp.concatenate([v[0].transpose(2, 1, 0, 3), v[1].transpose(2, 0, 1, 3)]).reshape(-1)

    def reference_order(v):
        v = v.reshape(4, 2, 4, 4, 4)
        return jnp.concatenate(
            [v[:2].transpose(3, 2, 0, 1, 4), v[2:].transpose(2, 3, 0, 1, 4)]
        ).reshape(-1)

    def from_reference_order(v):
        v = v.reshape(2, 4, 4, 2, 2, 4)
        return jnp.concatenate(
            [v[0].transpose(2, 3, 1, 0, 4), v[1].transpose(2, 3, 0, 1, 4)]
        ).reshape(-1)

    my_targets = mine(targets)
    p_targets = policy_order(my_targets)
    r_targets = reference_order(my_targets)
    active = mine(response_mask).astype(jnp.float32).reshape(-1)

    own = lax.dynamic_slice_in_dim(policy_hidden, (x * 4 + y) * 8, 8, 0)
    own = own.reshape(8, 4, 2, 512)
    first = jnp.where(c == 0, own[:, :, 0], own[:, :, 1]).reshape(8, 2048)
    second = jnp.where(c == 0, own[:, :, 1], own[:, :, 0]).reshape(8, 2048)
    own = jnp.concatenate([first, second], axis=1)
    far = swap(reference_hidden, "zh", 1)
    low = jnp.where(zh == 0, reference_hidden, far)
    high = jnp.where(zh == 0, far, reference_hidden)
    both = gathered_z(jnp.concatenate([own, low, high], axis=0))

    after = (both[3, 15, 4095].astype(jnp.float32) > 1e30).astype(jnp.int32)

    def entries(k):
        return lax.dynamic_slice_in_dim(policy_weight, ((zl ^ k) + after) * width, width, 1)

    pieces = [entries(0)] + [swap(entries(k), "zl", k) for k in (1, 2, 3)]
    near_weight = jnp.zeros((4, rows, width), jnp.bfloat16)
    for k, piece in enumerate(pieces):
        near_weight = lax.dynamic_update_slice_in_dim(near_weight, piece[None], zl ^ k, 0)
    near_weight = near_weight.reshape(4 * rows, width)
    far_weight = swap(near_weight, "c", 1)
    other_reference = swap(reference_weight, "c", 1)

    hidden, r_hidden = plane(both)

    logits = jnp.dot(
        hidden[:, :2048], near_weight, preferred_element_type=jnp.float32
    ) + jnp.dot(hidden[:, 2048:], far_weight, preferred_element_type=jnp.float32)
    vocab_index = zh * 16 + x * 4 + y
    offset = vocab_index * (4 * width) + zl * width
    policy_stats = head_stats(logits, p_targets, offset)
    powers = lax.optimization_barrier(
        jnp.exp(logits - policy_stats[0][:, None]).astype(jnp.bfloat16)
    )

    beside = swap(powers, "zl", 1)
    across = swap(powers, "zl", 2)
    both_away = swap(across, "zl", 1)

    reference_width = reference_weight.shape[1]
    near_logits = jnp.dot(r_hidden, reference_weight, preferred_element_type=jnp.float32)
    far_logits = jnp.dot(r_hidden, other_reference, preferred_element_type=jnp.float32)
    near_offset = ((zl * 2 + c) * 32 + vocab_index) * reference_width
    far_offset = ((zl * 2 + 1 - c) * 32 + vocab_index) * reference_width
    reference_stats = merge(
        head_stats(near_logits, r_targets, near_offset),
        head_stats(far_logits, r_targets, far_offset),
    )
    stats = policy_stats + reference_stats
    stats, tops = exchanged(stats, "zl", 1, (policy_stats[0],))
    tops = (policy_stats[0],) + tops
    stats, more = exchanged(stats, "zl", 2, tops)
    tops = tops + more
    for axis, k in (("x", 1), ("x", 2), ("y", 1), ("y", 2), ("zh", 1)):
        stats, _ = exchanged(stats, axis, k)

    policy_total = stats[0] + jnp.log(stats[1])
    reference_logp = stats[5] - stats[3] - jnp.log(stats[4])
    policy_logp = stats[2] - policy_total
    ratio = jnp.sum(
        (active * (from_policy_order(policy_logp) - from_reference_order(reference_logp))).reshape(
            16, 32
        ),
        axis=1,
    )
    far_ratio = swap(ratio, "c", 1)
    ratios = jnp.stack(
        [
            jnp.where(c == 0, ratio, far_ratio).reshape(4, 4),
            jnp.where(c == 0, far_ratio, ratio).reshape(4, 4),
        ],
        axis=1,
    ).reshape(32)
    total_loss, factor = pair_terms(ratios, pair_index)
    my_factor = lax.dynamic_index_in_dim(factor.reshape(4, 2, 4), c, 1, keepdims=False).reshape(16)
    token_scale = policy_order(active * jnp.repeat(my_factor, 32))

    at_target = token_scale * (1.0 - jnp.exp(policy_logp))
    whole = jnp.zeros((512, 4 * width), jnp.bfloat16)
    for k, piece in enumerate((powers, beside, across, both_away)):
        start = vocab_index * (4 * width) + (zl ^ k) * width
        ids = lax.broadcasted_iota(jnp.int32, piece.shape, 1)
        weight = token_scale * jnp.exp(tops[k] - policy_total)
        grad = jnp.where(
            ids == (p_targets - start)[:, None],
            at_target[:, None],
            -weight[:, None] * piece.astype(jnp.float32),
        ).astype(jnp.bfloat16)
        whole = lax.dynamic_update_slice_in_dim(whole, grad, (zl ^ k) * width, 1)
    grads = jnp.concatenate([whole, swap(whole, "c", 1)], axis=0)

    columns = lax.dynamic_slice_in_dim(hidden, zl * rows, rows, 1)
    far_columns = swap(lax.dynamic_slice_in_dim(hidden, 2048 + zl * rows, rows, 1), "c", 1)
    columns = jnp.concatenate([columns, far_columns], axis=0)

    part = lax.dot_general(
        grads, policy_weight, (((1,), (1,)), ((), ())), preferred_element_type=jnp.float32
    )
    part = part.reshape(2, 2, 4, 4, 2, 8, rows)
    near = jnp.where(c == 0, part[0], part[1])
    far = jnp.where(c == 0, part[1], part[0])

    def blocks_of(p):
        return jnp.stack([p[0].transpose(2, 1, 0, 3, 4), p[1].transpose(2, 0, 1, 3, 4)], axis=2)

    blocks = jnp.stack([blocks_of(near), blocks_of(far)], axis=1)
    blocks = blocks.reshape(16, 2, 32, rows)
    blocks = lax.all_to_all(blocks, ("x", "y"), 0, 0, tiled=True)
    summed = jnp.sum(blocks, axis=0)
    kept = lax.dynamic_index_in_dim(summed, zh, 0, keepdims=False)
    sent = lax.dynamic_index_in_dim(summed, 1 - zh, 0, keepdims=False)
    hidden_grad = (kept + swap(sent, "zh", 1)).astype(jnp.bfloat16)
    weight_grad = lax.dot_general(
        columns, grads, (((0,), (0,)), ((), ())), preferred_element_type=jnp.float32
    ).astype(jnp.bfloat16)
    return (hidden_grad, weight_grad, total_loss)


def solution(mesh):
    torus = Mesh(mesh.devices.reshape(4, 2, 2, 4, 4), AXES)
    in_specs = (P(DP, None), P(DP, VOCAB), P(DP_VOCAB, None), P(None, DP_VOCAB), P(), P(), P())
    out_specs = (P(VOCAB, DP), P(DP, VOCAB), P())
    return jax.shard_map(local, mesh=torus, in_specs=in_specs, out_specs=out_specs, check_vma=False)
```

```python
import jax
import jax.numpy as jnp
import numpy as np
from jax import lax
from jax.sharding import Mesh
from jax.sharding import PartitionSpec as P

AXES = ("zl", "c", "zh", "x", "y")
DP = ("zl", "c")
VOCAB = ("zh", "x", "y")
DP_VOCAB = ("zl", "c", "zh", "x", "y")
RING = ("zl", "zh")

beta = 0.1
loss_scale = 4096.0


def swap(value, axis, k):
    n = lax.axis_size(axis)
    return lax.ppermute(value, axis, [(i, i ^ k) for i in range(n)])


def from_ahead(value, axis, k):
    n = lax.axis_size(axis)
    return lax.ppermute(value, axis, [(i, (i - k) % n) for i in range(n)])


def from_z_ahead(value, k):
    at = lambda z: (z % 4) * 2 + z // 4
    return lax.ppermute(value, RING, [(at(z), at((z - k) % 8)) for z in range(8)])


def placed(pieces, first):
    out = jnp.zeros((4, *pieces[0].shape), pieces[0].dtype)
    for k, piece in enumerate(pieces):
        out = lax.dynamic_update_slice_in_dim(out, piece[None], (first + k) % 4, 0)
    return out


def gathered(value, axis):
    pieces = [value] + [from_ahead(value, axis, k) for k in (1, 2, 3)]
    return placed(pieces, lax.axis_index(axis))


def gathered_z(value):
    pieces = [value] + [from_z_ahead(value, k) for k in (1, 2, -1)]
    return placed(pieces, lax.axis_index("zl"))


def put(heads, colour, place, start, piece):
    return tuple(
        lax.dynamic_update_slice(
            head, piece[None, None, :, :, 8 * h : 8 * h + 8], (colour, place, start, 0, 0, 0)
        )
        for h, head in enumerate(heads)
    )


def plane(value):
    heads = tuple(jnp.zeros((2, 4, 4, 2, 8, value.shape[2]), value.dtype) for _ in range(2))
    rows = {0: gathered(value[:2], "x"), 1: gathered(value[2:], "y")}
    for colour, axis in ((0, "y"), (1, "x")):
        i = lax.axis_index(axis)
        row = rows[colour]
        ahead = from_ahead(row, axis, 1)
        behind = from_ahead(row, axis, 3)
        low, high = ahead[:2], behind[2:]
        far_low = from_ahead(low, axis, 1)
        far_high = from_ahead(high, axis, 3)
        heads = put(heads, colour, i, 0, row)
        heads = put(heads, colour, (i + 1) % 4, 0, ahead)
        heads = put(heads, colour, (i + 3) % 4, 0, behind)
        heads = put(heads, colour, (i + 2) % 4, 0, far_low)
        heads = put(heads, colour, (i + 2) % 4, 2, far_high)
    return tuple(head.reshape(512, -1) for head in heads)


def policy_order(v):
    xp = np if isinstance(v, np.ndarray) else jnp
    v = v.reshape(4, 4, 4, 8)
    return xp.concatenate([v[:2].transpose(2, 1, 0, 3), v[2:].transpose(1, 2, 0, 3)]).reshape(-1)


def reference_order(v):
    xp = np if isinstance(v, np.ndarray) else jnp
    v = v.reshape(4, 2, 4, 4, 4)
    return xp.concatenate(
        [v[:2].transpose(3, 2, 0, 1, 4), v[2:].transpose(2, 3, 0, 1, 4)]
    ).reshape(-1)


def head_stats(logits, targets, offset):
    top = jnp.max(logits, axis=1)
    exp_total = jnp.sum(jnp.exp(logits - top[:, None]), axis=1)
    ids = lax.broadcasted_iota(jnp.int32, logits.shape, 1)
    pick = jnp.sum(jnp.where(ids == (targets - offset)[:, None], logits, 0.0), axis=1)
    return (top, exp_total, pick)


def merge(a, b):
    top = jnp.maximum(a[0], b[0])
    return (top, a[1] * jnp.exp(a[0] - top) + b[1] * jnp.exp(b[0] - top), a[2] + b[2])


def merge_stacks(a, b):
    return jnp.stack(merge((a[0], a[1], a[2]), (b[0], b[1], b[2])))


def exchanged(stats, axis, k):
    return merge_stacks(stats, swap(stats, axis, k))


def local(
    policy_hidden,
    policy_weight,
    reference_hidden,
    reference_weight,
    targets,
    response_mask,
    pair_index,
):
    zl, c, zh, x, y = (lax.axis_index(a) for a in AXES)
    width = policy_weight.shape[1] // 4
    rows = policy_weight.shape[0]

    def mine(values):
        return lax.dynamic_index_in_dim(values.reshape(4, 2, 128), c, 1, keepdims=False)

    my_targets = mine(targets)
    my_active = mine(response_mask).astype(jnp.float32)
    p_targets, r_targets = policy_order(my_targets), reference_order(my_targets)
    p_active, r_active = policy_order(my_active), reference_order(my_active)
    counted = np.arange(512, dtype=np.int32) // 32
    sequences = np.arange(16, dtype=np.int32)
    p_member = jnp.asarray(policy_order(counted)[None, :] == sequences[:, None])
    r_member = jnp.asarray(reference_order(counted)[None, :] == sequences[:, None])
    number = jnp.asarray(sequences // 4 * 8 + sequences % 4) + c * 4
    is_chosen = pair_index[0::2][:, None] == number[None, :]
    is_rejected = pair_index[1::2][:, None] == number[None, :]

    own = lax.dynamic_slice_in_dim(policy_hidden, (x * 4 + y) * 8, 8, 0)
    own = own.reshape(8, 4, 2, 512)
    first = jnp.where(c == 0, own[:, :, 0], own[:, :, 1]).reshape(8, 2048)
    second = jnp.where(c == 0, own[:, :, 1], own[:, :, 0]).reshape(8, 2048)
    own = jnp.concatenate([first, second], axis=1)
    far = swap(reference_hidden, "zh", 1)
    low = jnp.where(zh == 0, reference_hidden, far)
    high = jnp.where(zh == 0, far, reference_hidden)
    both = gathered_z(jnp.concatenate([own, low, high], axis=0))

    mixed = [
        lax.dynamic_slice_in_dim(policy_weight, (zl ^ k) * width, width, 1) for k in range(4)
    ]
    pieces = mixed[:1] + [swap(mixed[k], "zl", k) for k in (1, 2, 3)]
    near_weight = jnp.zeros((4, rows, width), jnp.bfloat16)
    for k, piece in enumerate(pieces):
        near_weight = lax.dynamic_update_slice_in_dim(near_weight, piece[None], zl ^ k, 0)
    near_weight = near_weight.reshape(4 * rows, width)
    mixed = jnp.concatenate(mixed, axis=1)
    far_weight = swap(near_weight, "c", 1)
    other_reference = swap(reference_weight, "c", 1)

    hidden, r_hidden = plane(both)

    logits = jnp.dot(
        hidden[:, :2048], near_weight, preferred_element_type=jnp.float32
    ) + jnp.dot(hidden[:, 2048:], far_weight, preferred_element_type=jnp.float32)
    vocab_index = zh * 16 + x * 4 + y
    offset = vocab_index * (4 * width) + zl * width
    policy_stats = head_stats(logits, p_targets, offset)
    powers = lax.optimization_barrier(
        jnp.exp(logits - policy_stats[0][:, None]).astype(jnp.bfloat16)
    )

    beside = swap(powers, "zl", 1)
    across = swap(powers, "zl", 2)
    both_away = swap(across, "zl", 1)

    reference_width = reference_weight.shape[1]
    near_logits = jnp.dot(r_hidden, reference_weight, preferred_element_type=jnp.float32)
    far_logits = jnp.dot(r_hidden, other_reference, preferred_element_type=jnp.float32)
    near_offset = ((zl * 2 + c) * 32 + vocab_index) * reference_width
    far_offset = ((zl * 2 + 1 - c) * 32 + vocab_index) * reference_width
    reference_stats = merge(
        head_stats(near_logits, r_targets, near_offset),
        head_stats(far_logits, r_targets, far_offset),
    )
    stats = jnp.stack([jnp.stack(both) for both in zip(policy_stats, reference_stats)])
    line = [stats] + [swap(stats, "zl", k) for k in (1, 2, 3)]
    tops = [one[0, 0] for one in line]
    stats = merge_stacks(merge_stacks(line[0], line[1]), merge_stacks(line[2], line[3]))
    for axis, k in (("x", 1), ("x", 2), ("y", 1), ("y", 2), ("zh", 1)):
        stats = exchanged(stats, axis, k)

    totals = stats[0] + jnp.log(stats[1])
    logp = stats[2] - totals
    policy_total, policy_logp = totals[0], logp[0]
    ratio = jnp.sum(
        jnp.where(p_member, (p_active * policy_logp)[None, :], 0.0)
        - jnp.where(r_member, (r_active * logp[1])[None, :], 0.0),
        axis=1,
    )
    parts = jnp.sum(
        jnp.where(is_chosen, ratio[None, :], 0.0) - jnp.where(is_rejected, ratio[None, :], 0.0),
        axis=1,
    )
    margin = beta * (parts + swap(parts, "c", 1))
    pair_count = margin.shape[0]
    total_loss = jnp.sum(jax.nn.softplus(-margin)) / pair_count
    pair_weight = -beta * loss_scale * jax.nn.sigmoid(-margin) / pair_count
    factor = jnp.sum(
        jnp.where(is_chosen, pair_weight[:, None], 0.0)
        - jnp.where(is_rejected, pair_weight[:, None], 0.0),
        axis=0,
    )
    token_scale = p_active * jnp.sum(jnp.where(p_member, factor[:, None], 0.0), axis=0)

    at_target = token_scale * (1.0 - jnp.exp(policy_logp))
    whole = []
    for k, piece in enumerate((powers, beside, across, both_away)):
        start = vocab_index * (4 * width) + (zl ^ k) * width
        ids = lax.broadcasted_iota(jnp.int32, piece.shape, 1)
        weight = token_scale * jnp.exp(tops[k] - policy_total)
        grad = jnp.where(
            ids == (p_targets - start)[:, None],
            at_target[:, None],
            -weight[:, None] * piece.astype(jnp.float32),
        )
        whole.append(grad.astype(jnp.bfloat16))
    whole = jnp.concatenate(whole, axis=1)
    grads = jnp.concatenate([whole, swap(whole, "c", 1)], axis=0)

    columns = lax.dynamic_slice_in_dim(hidden, zl * rows, rows, 1)
    far_columns = swap(lax.dynamic_slice_in_dim(hidden, 2048 + zl * rows, rows, 1), "c", 1)
    columns = jnp.concatenate([columns, far_columns], axis=0)

    part = lax.dot_general(
        grads, mixed, (((1,), (1,)), ((), ())), preferred_element_type=jnp.float32
    )
    part = part.reshape(2, 2, 4, 4, 2, 8, rows)
    near = jnp.where(c == 0, part[0], part[1])
    far = jnp.where(c == 0, part[1], part[0])

    def blocks_of(p):
        return jnp.stack([p[0].transpose(2, 1, 0, 3, 4), p[1].transpose(2, 0, 1, 3, 4)], axis=2)

    blocks = jnp.stack([blocks_of(near), blocks_of(far)], axis=1)
    blocks = blocks.reshape(16, 2, 32, rows).astype(jnp.bfloat16)
    blocks = lax.all_to_all(blocks, ("x", "y"), 0, 0, tiled=True)
    summed = jnp.sum(blocks.astype(jnp.float32), axis=0)
    kept = lax.dynamic_index_in_dim(summed, zh, 0, keepdims=False)
    sent = lax.dynamic_index_in_dim(summed, 1 - zh, 0, keepdims=False)
    hidden_grad = (kept + swap(sent, "zh", 1)).astype(jnp.bfloat16)
    product = lax.dot_general(
        columns, grads, (((0,), (0,)), ((), ())), preferred_element_type=jnp.float32
    ).astype(jnp.bfloat16)
    weight_grad = jnp.zeros((rows, 4 * width), jnp.bfloat16)
    for k in range(4):
        weight_grad = lax.dynamic_update_slice_in_dim(
            weight_grad, product[:, k * width : (k + 1) * width], (zl ^ k) * width, 1
        )
    return (hidden_grad, weight_grad, total_loss)


def solution(mesh):
    torus = Mesh(mesh.devices.reshape(4, 2, 2, 4, 4), AXES)
    in_specs = (P(DP, None), P(DP, VOCAB), P(DP_VOCAB, None), P(None, DP_VOCAB), P(), P(), P())
    out_specs = (P(VOCAB, DP), P(DP, VOCAB), P())
    return jax.shard_map(local, mesh=torus, in_specs=in_specs, out_specs=out_specs, check_vma=False)
```

```python
import jax
import jax.numpy as jnp
import numpy as np
from jax import lax
from jax.sharding import Mesh
from jax.sharding import PartitionSpec as P

AXES = ("zl", "c", "zh", "x", "y")
DP = ("zl", "c")
VOCAB = ("zh", "x", "y")
DP_VOCAB = ("zl", "c", "zh", "x", "y")
RING = ("zl", "zh")

beta = 0.1
loss_scale = 4096.0


def swap(value, axis, k):
    n = lax.axis_size(axis)
    return lax.ppermute(value, axis, [(i, i ^ k) for i in range(n)])


def from_ahead(value, axis, k):
    n = lax.axis_size(axis)
    return lax.ppermute(value, axis, [(i, (i - k) % n) for i in range(n)])


def from_z(value, step):
    at = lambda z: (z % 8 % 4) * 2 + z % 8 // 4
    return lax.ppermute(value, RING, [(at(step(z)), at(z)) for z in range(8)])


def placed(pieces, first):
    out = jnp.zeros((4, *pieces[0].shape), pieces[0].dtype)
    for k, piece in enumerate(pieces):
        out = lax.dynamic_update_slice_in_dim(out, piece[None], (first + k) % 4, 0)
    return out


def gathered(value, axis):
    pieces = [value] + [from_ahead(value, axis, k) for k in (1, 2, 3)]
    return placed(pieces, lax.axis_index(axis))


def gathered_z(value):
    steps = (lambda z: z + 1, lambda z: z + 2 if z % 2 else z - 2, lambda z: z - 1)
    pieces = [value] + [from_z(value, step) for step in steps]
    return placed(pieces, lax.axis_index("zl"))


def put(heads, colour, place, start, piece):
    return tuple(
        lax.dynamic_update_slice(
            head, piece[None, None, :, :, 8 * h : 8 * h + 8], (colour, place, start, 0, 0, 0)
        )
        for h, head in enumerate(heads)
    )


def plane(value):
    heads = tuple(jnp.zeros((2, 4, 4, 2, 8, value.shape[2]), value.dtype) for _ in range(2))
    rows = {0: gathered(value[:2], "x"), 1: gathered(value[2:], "y")}
    for colour, axis in ((0, "y"), (1, "x")):
        i = lax.axis_index(axis)
        row = rows[colour]
        ahead = from_ahead(row, axis, 1)
        behind = from_ahead(row, axis, 3)
        low, high = ahead[:2], behind[2:]
        far_low = from_ahead(low, axis, 1)
        far_high = from_ahead(high, axis, 3)
        heads = put(heads, colour, i, 0, row)
        heads = put(heads, colour, (i + 1) % 4, 0, ahead)
        heads = put(heads, colour, (i + 3) % 4, 0, behind)
        heads = put(heads, colour, (i + 2) % 4, 0, far_low)
        heads = put(heads, colour, (i + 2) % 4, 2, far_high)
    return tuple(head.reshape(512, -1) for head in heads)


def policy_order(v):
    xp = np if isinstance(v, np.ndarray) else jnp
    v = v.reshape(4, 4, 4, 8)
    return xp.concatenate([v[:2].transpose(2, 1, 0, 3), v[2:].transpose(1, 2, 0, 3)]).reshape(-1)


def reference_order(v):
    xp = np if isinstance(v, np.ndarray) else jnp
    v = v.reshape(4, 2, 4, 4, 4)
    return xp.concatenate(
        [v[:2].transpose(3, 2, 0, 1, 4), v[2:].transpose(2, 3, 0, 1, 4)]
    ).reshape(-1)


def head_stats(logits, targets, offset):
    top = jnp.max(logits, axis=1)
    exp_total = jnp.sum(jnp.exp(logits - top[:, None]), axis=1)
    ids = lax.broadcasted_iota(jnp.int32, logits.shape, 1)
    pick = jnp.sum(jnp.where(ids + offset == targets[:, None], logits, 0.0), axis=1)
    return (top, exp_total, pick)


def merge(a, b):
    top = jnp.maximum(a[0], b[0])
    return (top, a[1] * jnp.exp(a[0] - top) + b[1] * jnp.exp(b[0] - top), a[2] + b[2])


def merge_stacks(a, b):
    return jnp.stack(merge((a[0], a[1], a[2]), (b[0], b[1], b[2])))


def exchanged(stats, axis, k):
    return merge_stacks(stats, swap(stats, axis, k))


def local(
    policy_hidden,
    policy_weight,
    reference_hidden,
    reference_weight,
    targets,
    response_mask,
    pair_index,
):
    zl, c, zh, x, y = (lax.axis_index(a) for a in AXES)
    width = policy_weight.shape[1] // 4
    rows = policy_weight.shape[0]

    places = np.arange(512, dtype=np.int32) // 128 * 256 + np.arange(512, dtype=np.int32) % 128
    places = np.concatenate([policy_order(places), reference_order(places)])
    spots = lax.broadcasted_iota(jnp.int32, (1024, 1024), 0)
    chosen = (spots == jnp.asarray(places)[None, :] + c * 128).astype(jnp.bfloat16)
    values = jnp.stack([targets // 256, targets % 256, response_mask]).astype(jnp.bfloat16)
    values = jnp.dot(values, chosen, preferred_element_type=jnp.float32)
    wanted = (values[0] * 256.0 + values[1]).astype(jnp.int32)
    p_targets, r_targets = wanted[:512], wanted[512:]
    p_active, r_active = values[2, :512], values[2, 512:]
    counted = np.arange(512, dtype=np.int32) // 32
    sequences = np.arange(16, dtype=np.int32)
    p_member = jnp.asarray(policy_order(counted)[None, :] == sequences[:, None])
    r_member = jnp.asarray(reference_order(counted)[None, :] == sequences[:, None])
    number = jnp.asarray(sequences // 4 * 8 + sequences % 4) + c * 4
    is_chosen = pair_index[0::2][:, None] == number[None, :]
    is_rejected = pair_index[1::2][:, None] == number[None, :]

    own = lax.dynamic_slice_in_dim(policy_hidden, (x * 4 + y) * 8, 8, 0)
    own = own.reshape(8, 4, 2, 512)
    first = jnp.where(c == 0, own[:, :, 0], own[:, :, 1]).reshape(8, 2048)
    second = jnp.where(c == 0, own[:, :, 1], own[:, :, 0]).reshape(8, 2048)
    own = jnp.concatenate([first, second], axis=1)
    far = swap(reference_hidden, "zh", 1)
    low = jnp.where(zh == 0, reference_hidden, far)
    high = jnp.where(zh == 0, far, reference_hidden)
    both = gathered_z(jnp.concatenate([own, low, high], axis=0))

    mixed = [lax.dynamic_slice_in_dim(policy_weight, (zl ^ k) * width, width, 1) for k in range(4)]
    pieces = mixed[:1] + [swap(mixed[k], "zl", k) for k in (1, 2, 3)]
    near_weight = jnp.zeros((4, rows, width), jnp.bfloat16)
    for k, piece in enumerate(pieces):
        near_weight = lax.dynamic_update_slice_in_dim(near_weight, piece[None], zl ^ k, 0)
    near_weight = near_weight.reshape(4 * rows, width)
    mixed = jnp.concatenate(mixed, axis=1)
    far_weight = swap(near_weight, "c", 1)
    other_reference = swap(reference_weight, "c", 1)

    hidden, r_hidden = plane(both)

    logits = jnp.dot(
        hidden[:, :2048], near_weight, preferred_element_type=jnp.float32
    ) + jnp.dot(hidden[:, 2048:], far_weight, preferred_element_type=jnp.float32)
    vocab_index = zh * 16 + x * 4 + y
    offset = vocab_index * (4 * width) + zl * width
    policy_stats = head_stats(logits, p_targets, offset)
    powers = lax.optimization_barrier(
        jnp.exp(logits - policy_stats[0][:, None]).astype(jnp.bfloat16)
    )

    beside = swap(powers, "zl", 1)
    across = swap(powers, "zl", 2)
    across = lax.optimization_barrier(jnp.where(zl >= 0, across, jnp.zeros_like(across)))
    both_away = swap(across, "zl", 1)

    reference_width = reference_weight.shape[1]
    near_logits = jnp.dot(r_hidden, reference_weight, preferred_element_type=jnp.float32)
    far_logits = jnp.dot(r_hidden, other_reference, preferred_element_type=jnp.float32)
    near_offset = ((zl * 2 + c) * 32 + vocab_index) * reference_width
    far_offset = ((zl * 2 + 1 - c) * 32 + vocab_index) * reference_width
    reference_stats = merge(
        head_stats(near_logits, r_targets, near_offset),
        head_stats(far_logits, r_targets, far_offset),
    )
    stats = jnp.stack([jnp.stack(both) for both in zip(policy_stats, reference_stats)])
    line = [stats] + [swap(stats, "zl", k) for k in (1, 2, 3)]
    tops = [one[0, 0] for one in line]
    stats = merge_stacks(merge_stacks(line[0], line[1]), merge_stacks(line[2], line[3]))
    plane_stats = lax.all_to_all(
        jnp.broadcast_to(stats[None], (16, *stats.shape)), ("x", "y"), 0, 0, tiled=True
    )
    top = jnp.max(plane_stats[:, 0], axis=0)
    exp_total = jnp.sum(plane_stats[:, 1] * jnp.exp(plane_stats[:, 0] - top[None]), axis=0)
    stats = jnp.stack([top, exp_total, jnp.sum(plane_stats[:, 2], axis=0)])
    stats = exchanged(stats, "zh", 1)

    totals = stats[0] + jnp.log(stats[1])
    logp = stats[2] - totals
    policy_total, policy_logp = totals[0], logp[0]
    ratio = jnp.sum(
        jnp.where(p_member, (p_active * policy_logp)[None, :], 0.0)
        - jnp.where(r_member, (r_active * logp[1])[None, :], 0.0),
        axis=1,
    )
    parts = jnp.sum(
        jnp.where(is_chosen, ratio[None, :], 0.0) - jnp.where(is_rejected, ratio[None, :], 0.0),
        axis=1,
    )
    margin = beta * (parts + swap(parts, "c", 1))
    pair_count = margin.shape[0]
    total_loss = jnp.sum(jax.nn.softplus(-margin)) / pair_count
    pair_weight = -beta * loss_scale * jax.nn.sigmoid(-margin) / pair_count
    factor = jnp.sum(
        jnp.where(is_chosen, pair_weight[:, None], 0.0)
        - jnp.where(is_rejected, pair_weight[:, None], 0.0),
        axis=0,
    )
    token_scale = p_active * jnp.sum(jnp.where(p_member, factor[:, None], 0.0), axis=0)

    at_target = token_scale * (1.0 - jnp.exp(policy_logp))
    whole = []
    for k, piece in enumerate((powers, beside, across, both_away)):
        start = vocab_index * (4 * width) + (zl ^ k) * width
        ids = lax.broadcasted_iota(jnp.int32, piece.shape, 1)
        weight = token_scale * jnp.exp(tops[k] - policy_total)
        grad = jnp.where(
            ids + start == p_targets[:, None],
            at_target[:, None],
            -weight[:, None] * piece.astype(jnp.float32),
        )
        whole.append(grad.astype(jnp.bfloat16))
    whole = jnp.concatenate(whole, axis=1)
    grads = jnp.concatenate([whole, swap(whole, "c", 1)], axis=0)

    columns = lax.dynamic_slice_in_dim(hidden, zl * rows, rows, 1)
    sent_columns = lax.dynamic_slice_in_dim(hidden, 2048 + zl * rows, rows, 1)
    far_columns = swap(sent_columns, "c", 1)
    columns = jnp.concatenate([columns, far_columns], axis=0)

    part = lax.dot_general(
        grads, mixed, (((1,), (1,)), ((), ())), preferred_element_type=jnp.float32
    )
    part = part.reshape(2, 2, 4, 4, 2, 8, rows)
    near = jnp.where(c == 0, part[0], part[1])
    far = jnp.where(c == 0, part[1], part[0])

    def blocks_of(p):
        return jnp.stack([p[0].transpose(2, 1, 0, 3, 4), p[1].transpose(2, 0, 1, 3, 4)], axis=2)

    blocks = jnp.stack([blocks_of(near), blocks_of(far)], axis=1)
    blocks = blocks.reshape(16, 2, 32, rows).astype(jnp.bfloat16)
    blocks = lax.all_to_all(blocks, ("x", "y"), 0, 0, tiled=True)
    summed = jnp.sum(blocks.astype(jnp.float32), axis=0)
    kept = lax.dynamic_index_in_dim(summed, zh, 0, keepdims=False)
    sent = lax.dynamic_index_in_dim(summed, 1 - zh, 0, keepdims=False)
    hidden_grad = (kept + swap(sent, "zh", 1)).astype(jnp.bfloat16)
    product = lax.dot_general(
        columns, grads, (((0,), (0,)), ((), ())), preferred_element_type=jnp.float32
    ).astype(jnp.bfloat16)
    weight_grad = jnp.zeros((rows, 4 * width), jnp.bfloat16)
    for k in range(4):
        weight_grad = lax.dynamic_update_slice_in_dim(
            weight_grad, product[:, k * width : (k + 1) * width], (zl ^ k) * width, 1
        )
    return (hidden_grad, weight_grad, total_loss)


def solution(mesh):
    torus = Mesh(mesh.devices.reshape(4, 2, 2, 4, 4), AXES)
    in_specs = (P(DP, None), P(DP, VOCAB), P(DP_VOCAB, None), P(None, DP_VOCAB), P(), P(), P())
    out_specs = (P(VOCAB, DP), P(DP, VOCAB), P())
    return jax.shard_map(local, mesh=torus, in_specs=in_specs, out_specs=out_specs, check_vma=False)
```

```python
import jax
import jax.numpy as jnp
import numpy as np
from jax import lax
from jax.sharding import Mesh
from jax.sharding import PartitionSpec as P

AXES = ("zl", "c", "zh", "x", "y")
DP = ("zl", "c")
VOCAB = ("zh", "x", "y")
DP_VOCAB = ("zl", "c", "zh", "x", "y")
RING = ("zl", "zh")

beta = 0.1
loss_scale = 4096.0


def swap(value, axis, k):
    n = lax.axis_size(axis)
    return lax.ppermute(value, axis, [(i, i ^ k) for i in range(n)])


def from_ahead(value, axis, k):
    n = lax.axis_size(axis)
    return lax.ppermute(value, axis, [(i, (i - k) % n) for i in range(n)])


def from_z(value, step):
    at = lambda z: (z % 8 % 4) * 2 + z % 8 // 4
    return lax.ppermute(value, RING, [(at(step(z)), at(z)) for z in range(8)])


def placed(pieces, first):
    out = jnp.zeros((4, *pieces[0].shape), pieces[0].dtype)
    for k, piece in enumerate(pieces):
        out = lax.dynamic_update_slice_in_dim(out, piece[None], (first + k) % 4, 0)
    return out


def gathered(value, axis):
    pieces = [value] + [from_ahead(value, axis, k) for k in (1, 2, 3)]
    return placed(pieces, lax.axis_index(axis))


def gathered_z(value):
    steps = (lambda z: z + 1, lambda z: z + 2 if z % 2 else z - 2, lambda z: z - 1)
    pieces = [value] + [from_z(value, step) for step in steps]
    return placed(pieces, lax.axis_index("zl"))


def put(heads, colour, place, start, piece):
    return tuple(
        lax.dynamic_update_slice(
            head, piece[None, None, :, :, 8 * h : 8 * h + 8], (colour, place, start, 0, 0, 0)
        )
        for h, head in enumerate(heads)
    )


def plane(value):
    heads = tuple(jnp.zeros((2, 4, 4, 2, 8, value.shape[2]), value.dtype) for _ in range(2))
    rows = {0: gathered(value[:2], "x"), 1: gathered(value[2:], "y")}
    for colour, axis in ((0, "y"), (1, "x")):
        i = lax.axis_index(axis)
        row = rows[colour]
        ahead = from_ahead(row, axis, 1)
        behind = from_ahead(row, axis, 3)
        low, high = ahead[:2], behind[2:]
        far_low = from_ahead(low, axis, 1)
        far_high = from_ahead(high, axis, 3)
        heads = put(heads, colour, i, 0, row)
        heads = put(heads, colour, (i + 1) % 4, 0, ahead)
        heads = put(heads, colour, (i + 3) % 4, 0, behind)
        heads = put(heads, colour, (i + 2) % 4, 0, far_low)
        heads = put(heads, colour, (i + 2) % 4, 2, far_high)
    return tuple(head.reshape(512, -1) for head in heads)


def policy_order(v):
    xp = np if isinstance(v, np.ndarray) else jnp
    v = v.reshape(4, 4, 4, 8)
    return xp.concatenate([v[:2].transpose(2, 1, 0, 3), v[2:].transpose(1, 2, 0, 3)]).reshape(-1)


def reference_order(v):
    xp = np if isinstance(v, np.ndarray) else jnp
    v = v.reshape(4, 2, 4, 4, 4)
    return xp.concatenate(
        [v[:2].transpose(3, 2, 0, 1, 4), v[2:].transpose(2, 3, 0, 1, 4)]
    ).reshape(-1)


def head_stats(logits, targets, offset):
    top = jnp.max(logits, axis=1)
    exp_total = jnp.sum(jnp.exp(logits - top[:, None]), axis=1)
    ids = lax.broadcasted_iota(jnp.int32, logits.shape, 1)
    pick = jnp.sum(jnp.where(ids + offset == targets[:, None], logits, 0.0), axis=1)
    return (top, exp_total, pick)


def merge(a, b):
    top = jnp.maximum(a[0], b[0])
    return (top, a[1] * jnp.exp(a[0] - top) + b[1] * jnp.exp(b[0] - top), a[2] + b[2])


def merge_stacks(a, b):
    return jnp.stack(merge((a[0], a[1], a[2]), (b[0], b[1], b[2])))


def exchanged(stats, axis, k):
    return merge_stacks(stats, swap(stats, axis, k))


def local(
    policy_hidden,
    policy_weight,
    reference_hidden,
    reference_weight,
    targets,
    response_mask,
    pair_index,
):
    zl, c, zh, x, y = (lax.axis_index(a) for a in AXES)
    width = policy_weight.shape[1] // 4
    rows = policy_weight.shape[0]

    places = np.arange(512, dtype=np.int32) // 128 * 256 + np.arange(512, dtype=np.int32) % 128
    places = np.concatenate([policy_order(places), reference_order(places)])
    spots = lax.broadcasted_iota(jnp.int32, (1024, 1024), 0)
    chosen = (spots == jnp.asarray(places)[None, :] + c * 128).astype(jnp.bfloat16)
    values = jnp.stack([targets // 256, targets % 256, response_mask]).astype(jnp.bfloat16)
    values = jnp.dot(values, chosen, preferred_element_type=jnp.float32)
    wanted = (values[0] * 256.0 + values[1]).astype(jnp.int32)
    p_targets, r_targets = wanted[:512], wanted[512:]
    p_active, r_active = values[2, :512], values[2, 512:]
    counted = np.arange(512, dtype=np.int32) // 32
    sequences = np.arange(16, dtype=np.int32)
    p_member = jnp.asarray(policy_order(counted)[None, :] == sequences[:, None])
    r_member = jnp.asarray(reference_order(counted)[None, :] == sequences[:, None])
    number = jnp.asarray(sequences // 4 * 8 + sequences % 4) + c * 4
    is_chosen = pair_index[0::2][:, None] == number[None, :]
    is_rejected = pair_index[1::2][:, None] == number[None, :]

    own = lax.dynamic_slice_in_dim(policy_hidden, (x * 4 + y) * 8, 8, 0)
    own = own.reshape(8, 4, 2, 512)
    first = jnp.where(c == 0, own[:, :, 0], own[:, :, 1]).reshape(8, 2048)
    second = jnp.where(c == 0, own[:, :, 1], own[:, :, 0]).reshape(8, 2048)
    own = jnp.concatenate([first, second], axis=1)
    far = swap(reference_hidden, "zh", 1)
    low = jnp.where(zh == 0, reference_hidden, far)
    high = jnp.where(zh == 0, far, reference_hidden)
    both = gathered_z(jnp.concatenate([own, low, high], axis=0))

    mixed = [lax.dynamic_slice_in_dim(policy_weight, (zl ^ k) * width, width, 1) for k in range(4)]
    pieces = mixed[:1] + [swap(mixed[k], "zl", k) for k in (1, 2, 3)]
    near_weight = jnp.zeros((4, rows, width), jnp.bfloat16)
    for k, piece in enumerate(pieces):
        near_weight = lax.dynamic_update_slice_in_dim(near_weight, piece[None], zl ^ k, 0)
    near_weight = near_weight.reshape(4 * rows, width)
    mixed = jnp.concatenate(mixed, axis=1)
    far_weight = swap(near_weight, "c", 1)
    other_reference = swap(reference_weight, "c", 1)

    hidden, r_hidden = plane(both)

    logits = jnp.dot(
        hidden[:, :2048], near_weight, preferred_element_type=jnp.float32
    ) + jnp.dot(hidden[:, 2048:], far_weight, preferred_element_type=jnp.float32)
    vocab_index = zh * 16 + x * 4 + y
    offset = vocab_index * (4 * width) + zl * width
    policy_stats = head_stats(logits, p_targets, offset)
    powers = lax.optimization_barrier(
        jnp.exp(logits - policy_stats[0][:, None]).astype(jnp.bfloat16)
    )

    beside = swap(powers, "zl", 1)
    across = swap(powers, "zl", 2)
    across = lax.optimization_barrier(jnp.where(zl >= 0, across, jnp.zeros_like(across)))
    both_away = swap(across, "zl", 1)

    reference_width = reference_weight.shape[1]
    near_logits = jnp.dot(r_hidden, reference_weight, preferred_element_type=jnp.float32)
    far_logits = jnp.dot(r_hidden, other_reference, preferred_element_type=jnp.float32)
    near_offset = ((zl * 2 + c) * 32 + vocab_index) * reference_width
    far_offset = ((zl * 2 + 1 - c) * 32 + vocab_index) * reference_width
    reference_stats = merge(
        head_stats(near_logits, r_targets, near_offset),
        head_stats(far_logits, r_targets, far_offset),
    )
    stats = jnp.stack([jnp.stack(both) for both in zip(policy_stats, reference_stats)])
    line = [stats] + [swap(stats, "zl", k) for k in (1, 2, 3)]
    tops = [one[0, 0] for one in line]
    stats = merge_stacks(merge_stacks(line[0], line[1]), merge_stacks(line[2], line[3]))
    plane_stats = lax.all_to_all(
        jnp.broadcast_to(stats[None], (16, *stats.shape)), ("x", "y"), 0, 0, tiled=True
    )
    top = jnp.max(plane_stats[:, 0], axis=0)
    exp_total = jnp.sum(plane_stats[:, 1] * jnp.exp(plane_stats[:, 0] - top[None]), axis=0)
    stats = jnp.stack([top, exp_total, jnp.sum(plane_stats[:, 2], axis=0)])
    stats = exchanged(stats, "zh", 1)

    totals = stats[0] + jnp.log(stats[1])
    logp = stats[2] - totals
    policy_total, policy_logp = totals[0], logp[0]
    ratio = jnp.sum(
        jnp.where(p_member, (p_active * policy_logp)[None, :], 0.0)
        - jnp.where(r_member, (r_active * logp[1])[None, :], 0.0),
        axis=1,
    )
    parts = jnp.sum(
        jnp.where(is_chosen, ratio[None, :], 0.0) - jnp.where(is_rejected, ratio[None, :], 0.0),
        axis=1,
    )
    margin = beta * (parts + swap(parts, "c", 1))
    pair_count = margin.shape[0]
    total_loss = jnp.sum(jax.nn.softplus(-margin)) / pair_count
    pair_weight = -beta * loss_scale * jax.nn.sigmoid(-margin) / pair_count
    factor = jnp.sum(
        jnp.where(is_chosen, pair_weight[:, None], 0.0)
        - jnp.where(is_rejected, pair_weight[:, None], 0.0),
        axis=0,
    )
    token_scale = p_active * jnp.sum(jnp.where(p_member, factor[:, None], 0.0), axis=0)

    at_target = token_scale * (1.0 - jnp.exp(policy_logp))
    whole = []
    for k, piece in enumerate((powers, beside, across, both_away)):
        start = vocab_index * (4 * width) + (zl ^ k) * width
        ids = lax.broadcasted_iota(jnp.int32, piece.shape, 1)
        weight = token_scale * jnp.exp(tops[k] - policy_total)
        grad = jnp.where(
            ids + start == p_targets[:, None],
            at_target[:, None],
            -weight[:, None] * piece.astype(jnp.float32),
        )
        whole.append(grad.astype(jnp.bfloat16))
    whole = jnp.concatenate(whole, axis=1)
    other = swap(whole, "c", 1)

    columns = lax.dynamic_slice_in_dim(hidden, zl * rows, rows, 1)
    sent_columns = lax.dynamic_slice_in_dim(hidden, 2048 + zl * rows, rows, 1)
    far_columns = swap(sent_columns, "c", 1)
    columns = jnp.concatenate([columns, far_columns], axis=0)

    def hidden_of(grad):
        part = lax.dot_general(
            grad, mixed, (((1,), (1,)), ((), ())), preferred_element_type=jnp.float32
        )
        return part.astype(jnp.bfloat16).reshape(2, 4, 4, 2, 8, rows)

    near_part = lax.optimization_barrier(hidden_of(whole))
    far_part = hidden_of(other)
    grads = jnp.concatenate([whole, other], axis=0)
    near = jnp.where(c == 0, near_part, far_part)
    far = jnp.where(c == 0, far_part, near_part)

    def blocks_of(p):
        return jnp.stack([p[0].transpose(2, 1, 0, 3, 4), p[1].transpose(2, 0, 1, 3, 4)], axis=2)

    blocks = jnp.stack([blocks_of(near), blocks_of(far)], axis=1)
    blocks = blocks.reshape(16, 2, 32, rows)
    blocks = lax.all_to_all(blocks, ("x", "y"), 0, 0, tiled=True)
    summed = jnp.sum(blocks.astype(jnp.float32), axis=0)
    kept = lax.dynamic_index_in_dim(summed, zh, 0, keepdims=False)
    sent = lax.dynamic_index_in_dim(summed, 1 - zh, 0, keepdims=False)
    hidden_grad = (kept + swap(sent, "zh", 1)).astype(jnp.bfloat16)
    product = lax.dot_general(
        columns, grads, (((0,), (0,)), ((), ())), preferred_element_type=jnp.float32
    ).astype(jnp.bfloat16)
    weight_grad = jnp.zeros((rows, 4 * width), jnp.bfloat16)
    for k in range(4):
        weight_grad = lax.dynamic_update_slice_in_dim(
            weight_grad, product[:, k * width : (k + 1) * width], (zl ^ k) * width, 1
        )
    return (hidden_grad, weight_grad, total_loss)


def solution(mesh):
    torus = Mesh(mesh.devices.reshape(4, 2, 2, 4, 4), AXES)
    in_specs = (P(DP, None), P(DP, VOCAB), P(DP_VOCAB, None), P(None, DP_VOCAB), P(), P(), P())
    out_specs = (P(VOCAB, DP), P(DP, VOCAB), P())
    return jax.shard_map(local, mesh=torus, in_specs=in_specs, out_specs=out_specs, check_vma=False)
```
